768 devices in a mesh: dp: 48 (over y_lo, z), mp: 16 (over y_hi, x, core).
Axes of the slice: x: 4, y: 8 (y_hi: 2, y_lo: 4; y = y_hi * 4 + y_lo), z: 12, core: 2. Of those that a mesh axis runs over, the one named last changes fastest.
Arguments:
- output_gradient: bfloat16 [9216, 3584], P('dp', 'mp'), may hold values from -6 to 6
- gate_preactivation: bfloat16 [9216, 9984], P('dp', 'mp'), may hold values from -8 to 8
- up_preactivation: bfloat16 [9216, 9984], P('dp', 'mp'), may hold values from -6 to 6
- down_weight: bfloat16 [9984, 3584], P('mp'), may hold values from -0.0625 to 0.0625
- adapter_first: bfloat16 [9984, 96], P('mp'), may hold values from -0.0625 to 0.0625
- adapter_second: bfloat16 [96, 3584], replicated, may hold values from -0.09375 to 0.09375
- plan: int32 [1152], P('dp'), may hold values from 0 to 47, as said below
Outputs:
- grad_gate: bfloat16 [9216, 9984], P('dp', 'mp')
- grad_up: bfloat16 [9216, 9984], P('dp', 'mp')
- grad_a: float32 [16, 624, 96], P('mp', 'dp')
- grad_b: float32 [96, 3584], P('dp')
The draws below stay inside these ranges and needn't reach their ends.
Inputs may be any that keep to these rules, and one draw needn't show every extreme that they name: Every owner 0 to 47 is named by exactly 24 blocks; of the 24 blocks of one device (plan rows of one index of dp) at most 1 name the same owner, and in every draw some device's blocks name one owner exactly 1 times.
All inputs are finite; a program needn't handle non-finite values.
Results may differ from the reference program's by a relative error of at most 0.005.
Values may be sent and summed in bfloat16 or wider, within the bound.
A program may use at most 32 MiB of HBM per device.

```python
import jax
import jax.numpy as jnp
from jax import lax

MODEL_WIDTH = 3584
HIDDEN_SHARE = 9984
ADAPTER_RANK = 96
OWN = 24
CAP = 1
TOKENS = 9216
N_DP = 48
N_MP = 16


def draw_plan(key, part):
    key_shift = jax.random.fold_in(key, 11)
    key_slots = jax.random.fold_in(key, 23)
    key_label = jax.random.fold_in(key, 37)
    shift_order = jax.random.permutation(key_shift, N_DP)
    shifts = shift_order[jnp.arange(OWN) // CAP]
    slot_keys = jax.random.split(key_slots, N_DP)
    slot_perm = jax.vmap(lambda single: jax.random.permutation(single, OWN))(slot_keys)
    relabel = jax.random.permutation(key_label, N_DP)
    sources = jnp.arange(N_DP)[:, None]
    virtual = (sources + shifts[slot_perm]) % N_DP
    owners = relabel[virtual]
    return owners.reshape(-1).astype(jnp.int32)


def steps_of(own_key, extent, shards, smallest, largest):
    def one(axis_at, blocks):
        steps = jax.random.uniform(jax.random.fold_in(jax.random.fold_in(own_key, 6), axis_at), (blocks,), jnp.float32, smallest / len(shards), largest / len(shards))
        return jnp.repeat(jnp.exp(steps), extent[axis_at] // blocks).reshape((-1,) + (1,) * (len(extent) - axis_at - 1))

    loudness = one(*shards[0])
    for cut in shards[1:]:
        loudness = loudness * one(*cut)
    return loudness


def centred(stream_key, dims, spread, most, cuts=(), held_as=jnp.bfloat16):
    values = jax.random.normal(stream_key, dims, jnp.float32) * spread
    if len(cuts) > 0:
        values = steps_of(stream_key, dims, cuts, -0.22, 0.18) * values
    return jnp.clip(values, min=-most, max=most).astype(held_as)


def setup_inputs(seed: int = 0) -> dict:
    streams_of = jax.random.split(jax.random.key(seed), 8)
    output_gradient = centred(streams_of[0], (TOKENS, MODEL_WIDTH), 1.0, 6.0, ((0, 48), (1, 16)))
    gate_preactivation = centred(streams_of[1], (TOKENS, HIDDEN_SHARE), 1.5, 8.0, ((0, 48), (1, 16)))
    up_preactivation = centred(streams_of[2], (TOKENS, HIDDEN_SHARE), 1.0, 6.0, ((0, 48), (1, 16)))
    down_weight = centred(streams_of[3], (HIDDEN_SHARE, MODEL_WIDTH), HIDDEN_SHARE ** -0.5, 0.0625, ((0, 16),))
    adapter_first = centred(streams_of[4], (HIDDEN_SHARE, ADAPTER_RANK), HIDDEN_SHARE ** -0.5, 0.0625, ((0, 16),))
    adapter_second = centred(streams_of[5], (ADAPTER_RANK, MODEL_WIDTH), MODEL_WIDTH ** -0.5, 0.09375)
    plan = draw_plan(jax.random.fold_in(streams_of[7], 71), 0)
    return dict(output_gradient=output_gradient, gate_preactivation=gate_preactivation, up_preactivation=up_preactivation, down_weight=down_weight, adapter_first=adapter_first, adapter_second=adapter_second, plan=plan)


def reference(output_gradient, gate_preactivation, up_preactivation, down_weight, adapter_first, adapter_second, plan):
    block_count = plan.shape[0]
    owned = block_count // N_DP
    block_index = jnp.arange(block_count, dtype=jnp.int32)
    same_owner = (plan[None, :] == plan[:, None]) & (block_index[None, :] < block_index[:, None])
    rank_in = jnp.sum(same_owner.astype(jnp.int32), axis=1).astype(jnp.int32)
    target = (plan * owned + rank_in).astype(jnp.int32)
    blocks_of = output_gradient.reshape(block_count, -1)
    packed_tokens = jnp.zeros_like(blocks_of).at[target].set(blocks_of).reshape(output_gradient.shape)
    gate_vals = gate_preactivation.astype(jnp.float32)
    up_vals = up_preactivation.astype(jnp.float32)
    sigmoid_gate = jax.nn.sigmoid(gate_vals)
    silu_gate = gate_vals * sigmoid_gate
    hidden_units = (silu_gate * up_vals).astype(jnp.bfloat16)
    low_rank_rows = jnp.dot(hidden_units, adapter_first, preferred_element_type=jnp.float32).astype(jnp.bfloat16)
    passed_through = lax.dot_general(packed_tokens, adapter_second, (((1,), (1,)), ((), ())), preferred_element_type=jnp.float32).astype(jnp.bfloat16)
    hidden_gradient = lax.dot_general(packed_tokens, down_weight, (((1,), (1,)), ((), ())), preferred_element_type=jnp.float32)
    hidden_gradient = hidden_gradient + lax.dot_general(passed_through, adapter_first, (((1,), (1,)), ((), ())), preferred_element_type=jnp.float32)
    grad_gate = (hidden_gradient * up_vals * sigmoid_gate * (1.0 + gate_vals * (1.0 - sigmoid_gate))).astype(jnp.bfloat16)
    grad_up = (hidden_gradient * silu_gate).astype(jnp.bfloat16)
    grad_a = lax.dot_general(hidden_units, passed_through, (((0,), (0,)), ((), ())), preferred_element_type=jnp.float32)
    grad_b = lax.dot_general(low_rank_rows, packed_tokens, (((0,), (0,)), ((), ())), preferred_element_type=jnp.float32)
    return grad_gate, grad_up, grad_a.reshape(N_MP, -1, grad_a.shape[1]), grad_b
```

```python
import jax
import jax.numpy as jnp
from jax import lax
from jax.experimental import pallas as pl
from jax.experimental.pallas import tpu as pltpu
from jax.sharding import PartitionSpec as P

MESH = pl.DeviceIdType.MESH
F32, BF16 = jnp.float32, jnp.bfloat16
DP, MP = 48, 16
TOK, FEAT, WIDE = 192, 224, 256
HID, RANK, RW = 624, 96, 128
PIECE = 13
MODEL = 3584


def dot_nn(a, b):
    return lax.dot_general(a, b, (((1,), (0,)), ((), ())), preferred_element_type=F32)


def dot_nt(a, b):
    return lax.dot_general(a, b, (((1,), (1,)), ((), ())), preferred_element_type=F32)


def dot_tn(a, b):
    return lax.dot_general(a, b, (((0,), (0,)), ((), ())), preferred_element_type=F32)


def iota(shape, dim):
    return lax.broadcasted_iota(jnp.int32, shape, dim)


def onehot(cond):
    return jnp.where(cond, 1.0, 0.0).astype(BF16)


def wait_bytes(ref, sem):
    pltpu.make_async_copy(ref, ref, sem).wait()


def kernel(
    og_hbm, gate_hbm, up_hbm, w_hbm, a1_hbm, a2_hbm, plan_hbm,
    gg_hbm, gu_hbm, ga_ref, gb_ref,
    og, og_ext, gate, up, w, a1, a2, plan,
    slots_out, slots_in, low_out, low_in, low_all,
    chunks, weights, acc, c_gate, c_up, hidden_t, earlier, gg, gu,
    b_part, b_out, b_in, b_all, a_out, a_in,
    load_sem, store_sem, g_recv, sems,
):
    me, mm = lax.axis_index("dp"), lax.axis_index("mp")
    (p_send, p_recv, l_send, l_recv, lg_send, lg_recv, g_send, b_send, b_recv,
     bg_send, bg_recv, r_send, r_recv) = [sems.at[k] for k in range(13)]

    barrier = pltpu.get_barrier_semaphore()

    @pl.loop(1, DP)
    def _(i):
        pl.semaphore_signal(
            barrier, inc=1, device_id={"dp": lax.rem(me + i, DP)}, device_id_type=MESH
        )

    @pl.loop(1, MP)
    def _(i):
        pl.semaphore_signal(
            barrier, inc=1, device_id={"mp": lax.rem(mm + i, MP)}, device_id_type=MESH
        )

    loads = [
        pltpu.make_async_copy(src, dst, load_sem.at[k])
        for k, (src, dst) in enumerate(
            [(plan_hbm, plan), (og_hbm, og), (gate_hbm, gate), (up_hbm, up),
             (a1_hbm, a1), (a2_hbm, a2), (w_hbm, w)]
        )
    ]
    for copy in loads:
        copy.start()

    def exchange(axis, count, mine, src, dst, send_sem, recv_sem, by_peer):
        @pl.loop(1, count)
        def _(i):
            peer = lax.rem(mine + i, count)
            pltpu.make_async_remote_copy(
                src_ref=src.at[peer] if by_peer else src.at[mine],
                dst_ref=dst.at[mine],
                send_sem=send_sem,
                recv_sem=recv_sem,
                device_id={axis: peer},
                device_id_type=MESH,
            ).start()

    loads[0].wait()
    expand = onehot(iota((24, TOK), 0) == (iota((24, TOK), 1) >> 3))
    plan_rows = jnp.broadcast_to(plan[...].astype(F32), (8, 24)).astype(BF16)
    owner_of = dot_nn(plan_rows, expand)[0:1, :]
    place = (iota((DP * 8, TOK), 0) >> 3).astype(F32)
    same_row = (iota((DP * 8, TOK), 0) & 7) == (iota((DP * 8, TOK), 1) & 7)
    sending = onehot((owner_of == place) & same_row)
    loads[1].wait()
    og_ext[:, :FEAT] = og[...]
    og_ext[:, FEAT:] = jnp.ones((TOK, WIDE - FEAT), BF16)
    slots_out[...] = dot_nn(sending, og_ext[...]).astype(BF16).reshape(DP, 8, WIDE)
    slots_in[me] = slots_out[me]

    pl.semaphore_wait(barrier, DP - 1 + MP - 1)
    exchange("dp", DP, me, slots_out, slots_in, p_send, p_recv, True)

    loads[2].wait()
    loads[3].wait()
    g = gate[...].astype(F32)
    u = up[...].astype(F32)
    sig = jax.nn.sigmoid(g)
    silu = g * sig
    c_up[...] = silu
    c_gate[...] = u * sig * (1.0 + g * (1.0 - sig))
    hidden = (silu * u).astype(BF16)
    loads[4].wait()
    low_out[...] = jnp.zeros((MP, 16, RW), F32)
    low_out[0 : TOK // 16, :, :RANK] = dot_nn(hidden, a1[...]).reshape(TOK // 16, 16, RANK)
    low_in[mm] = low_out[mm]
    exchange("mp", MP, mm, low_out, low_in, l_send, l_recv, True)

    row = iota((DP * 16, HID), 0)
    spread = onehot(((row >> 4) * PIECE + (row & 15) == iota((DP * 16, HID), 1)) & ((row & 15) < PIECE))
    hidden_t[...] = dot_nt(spread, hidden).astype(BF16)
    first = iota((DP * 8, DP * 8), 0)
    earlier[...] = onehot(((first >> 3) < (iota((DP * 8, DP * 8), 1) >> 3)) & ((first & 7) == 0))

    loads[5].wait()
    loads[6].wait()
    for k in range(MP):
        cols = slice(k * FEAT, (k + 1) * FEAT)
        weights[k, RANK:RW, :] = jnp.zeros((RW - RANK, WIDE), BF16)
        weights[k, :, FEAT:] = jnp.zeros((RW + HID, WIDE - FEAT), BF16)
        weights[k, 0:RANK, :FEAT] = a2[:, cols]
        weights[k, RW:, :FEAT] = w[:, cols]

    wait_bytes(low_in.at[pl.ds(0, MP - 1)], l_recv)
    low_all[mm] = jnp.sum(low_in[...], axis=0).astype(BF16)
    exchange("mp", MP, mm, low_all, low_all, lg_send, lg_recv, False)

    wait_bytes(slots_in.at[pl.ds(0, DP - 1)], p_recv)
    arrived = slots_in[...].reshape(DP * 8, WIDE)
    pick = onehot(iota((8, WIDE), 1) == FEAT)
    present = dot_nt(pick, arrived)
    rank = dot_nn(present.astype(BF16), earlier[...])
    place = (iota((TOK, DP * 8), 0) >> 3).astype(F32)
    same_row = (iota((TOK, DP * 8), 0) & 7) == (iota((TOK, DP * 8), 1) & 7)
    keeping = onehot((present[0:1, :] > 0.5) & (rank[0:1, :] == place) & same_row)
    packed = dot_nn(keeping, arrived).astype(BF16)
    chunks[mm] = packed

    h, x, c = mm // 8, lax.rem(mm // 2, 4), lax.rem(mm, 2)
    o, s = 1 - h, 1 - c
    ahead = lax.rem(x + 5 - 2 * c, 4)
    behind = lax.rem(x + 3 + 2 * c, 4)
    across = lax.rem(x + 2, 4)

    def at(hh, xx, cc):
        return hh * 8 + xx * 2 + cc

    def send(slot, dest):
        pltpu.make_async_remote_copy(
            src_ref=chunks.at[slot],
            dst_ref=chunks.at[slot],
            send_sem=g_send,
            recv_sem=g_recv.at[slot],
            device_id={"mp": dest},
            device_id_type=MESH,
        ).start()

    def arrive(slot):
        wait_bytes(chunks.at[slot], g_recv.at[slot])

    def consume(slot):
        acc[...] += dot_nt(chunks[slot], weights[slot])

    sibling = at(h, x, s)
    send(mm, at(o, x, c))
    send(mm, at(h, ahead, c))
    send(mm, at(h, behind, c))
    send(mm, sibling)
    acc[...] = dot_nt(chunks[mm], weights[mm])

    wait_bytes(low_all.at[pl.ds(0, MP - 1)], lg_recv)
    low = low_all[...].reshape(MP * 16, RW)[:TOK, :]
    b_part[...] = dot_tn(low, packed)
    for k in range(DP):
        b_out[k] = b_part[2 * k : 2 * k + 2, :]
    b_in[me] = b_out[me]
    exchange("dp", DP, me, b_out, b_in, b_send, b_recv, True)

    for hh in (h, o):
        if hh is o:
            arrive(at(o, x, c))
            send(at(o, x, c), at(h, ahead, c))
            send(at(o, x, c), at(h, behind, c))
            send(at(o, x, c), sibling)
            consume(at(o, x, c))
        arrive(at(hh, behind, c))
        send(at(hh, behind, c), at(h, ahead, c))
        send(at(hh, behind, c), sibling)
        consume(at(hh, behind, c))
        arrive(at(hh, ahead, c))
        send(at(hh, ahead, c), sibling)
        consume(at(hh, ahead, c))
        arrive(at(hh, across, c))
        send(at(hh, across, c), sibling)
        consume(at(hh, across, c))
        for xx in (x, ahead, behind, across):
            arrive(at(hh, xx, s))
            consume(at(hh, xx, s))

    through = acc[:, 0:RW].astype(BF16)
    a_out[...] = dot_nn(hidden_t[...], through).astype(BF16).reshape(DP, 16, RW)
    a_in[me] = a_out[me]
    exchange("dp", DP, me, a_out, a_in, r_send, r_recv, True)

    wait_bytes(b_in.at[pl.ds(0, DP - 1)], b_recv)
    b_all[mm] = jnp.sum(b_in[...], axis=0)
    exchange("mp", MP, mm, b_all, b_all, bg_send, bg_recv, False)

    grad_hidden = acc[:, RW:] + dot_nt(through[:, :RANK], a1[...])
    gg[...] = (grad_hidden * c_gate[...]).astype(BF16)
    gu[...] = (grad_hidden * c_up[...]).astype(BF16)
    stores = [
        pltpu.make_async_copy(gg, gg_hbm, store_sem.at[0]),
        pltpu.make_async_copy(gu, gu_hbm, store_sem.at[1]),
    ]
    for copy in stores:
        copy.start()

    wait_bytes(b_all.at[pl.ds(0, MP - 1)], bg_recv)
    for k in range(MP):
        gb_ref[:, k * FEAT : (k + 1) * FEAT] = b_all[k][:, :FEAT]

    wait_bytes(slots_out.at[pl.ds(0, DP - 1)], p_send)
    wait_bytes(low_out.at[pl.ds(0, MP - 1)], l_send)
    wait_bytes(low_all.at[pl.ds(0, MP - 1)], lg_send)
    wait_bytes(chunks.at[pl.ds(0, MP - 1)], g_send)
    wait_bytes(b_out.at[pl.ds(0, DP - 1)], b_send)
    wait_bytes(b_all.at[pl.ds(0, MP - 1)], bg_send)
    for copy in stores:
        copy.wait()
    wait_bytes(a_in.at[pl.ds(0, DP - 1)], r_recv)
    total = jnp.sum(a_in[...].astype(F32), axis=0)
    ga_ref[0] = total[:PIECE, :RANK]
    wait_bytes(a_out.at[pl.ds(0, DP - 1)], r_send)


def body(og, gate, up, w, a1, a2, plan):
    hbm = pl.BlockSpec(memory_space=pl.ANY)
    vmem = pl.BlockSpec(memory_space=pltpu.VMEM)
    V = pltpu.VMEM
    return tuple(pl.pallas_call(
        kernel,
        out_shape=(
            jax.ShapeDtypeStruct((TOK, HID), BF16),
            jax.ShapeDtypeStruct((TOK, HID), BF16),
            jax.ShapeDtypeStruct((1, PIECE, RANK), F32),
            jax.ShapeDtypeStruct((2, MODEL), F32),
        ),
        in_specs=[hbm] * 7,
        out_specs=(hbm, hbm, vmem, vmem),
        scratch_shapes=[
            V((TOK, FEAT), BF16),
            V((TOK, WIDE), BF16),
            V((TOK, HID), BF16),
            V((TOK, HID), BF16),
            V((HID, MODEL), BF16),
            V((HID, RANK), BF16),
            V((RANK, MODEL), BF16),
            V((1, 24), jnp.int32),
            V((DP, 8, WIDE), BF16),
            V((DP, 8, WIDE), BF16),
            V((MP, 16, RW), F32),
            V((MP, 16, RW), F32),
            V((MP, 16, RW), BF16),
            V((MP, TOK, WIDE), BF16),
            V((MP, RW + HID, WIDE), BF16),
            V((TOK, RW + HID), F32),
            V((TOK, HID), F32),
            V((TOK, HID), F32),
            V((DP * 16, TOK), BF16),
            V((DP * 8, DP * 8), BF16),
            V((TOK, HID), BF16),
            V((TOK, HID), BF16),
            V((RW, WIDE), F32),
            V((DP, 2, WIDE), F32),
            V((DP, 2, WIDE), F32),
            V((MP, 2, WIDE), F32),
            V((DP, 16, RW), BF16),
            V((DP, 16, RW), BF16),
            pltpu.SemaphoreType.DMA((7,)),
            pltpu.SemaphoreType.DMA((2,)),
            pltpu.SemaphoreType.DMA((MP,)),
            pltpu.SemaphoreType.DMA((13,)),
        ],
        compiler_params=pltpu.CompilerParams(
            collective_id=0, has_side_effects=True, vmem_limit_bytes=48 * 1024 * 1024
        ),
        name="repack_backward",
    )(og, gate, up, w, a1, a2, plan.reshape(1, 24)))


def solution(mesh):
    return jax.shard_map(
        body,
        mesh=mesh,
        in_specs=(
            P("dp", "mp"),
            P("dp", "mp"),
            P("dp", "mp"),
            P("mp", None),
            P("mp", None),
            P(),
            P("dp"),
        ),
        out_specs=(P("dp", "mp"), P("dp", "mp"), P("mp", "dp", None), P("dp", None)),
        check_vma=False,
    )
```

```python
import jax
import jax.numpy as jnp
from jax import lax
from jax.experimental import pallas as pl
from jax.experimental.pallas import tpu as pltpu
from jax.sharding import PartitionSpec as P

MESH = pl.DeviceIdType.MESH
F32, BF16 = jnp.float32, jnp.bfloat16
DP, MP = 48, 16
TOK, FEAT, WIDE = 192, 224, 256
HID, RANK, RW = 624, 96, 128
PIECE = 13
NY, NZ = 4, 12
MODEL = 3584


def dot_nn(a, b):
    return lax.dot_general(a, b, (((1,), (0,)), ((), ())), preferred_element_type=F32)


def dot_nt(a, b):
    return lax.dot_general(a, b, (((1,), (1,)), ((), ())), preferred_element_type=F32)


def dot_tn(a, b):
    return lax.dot_general(a, b, (((0,), (0,)), ((), ())), preferred_element_type=F32)


def iota(shape, dim):
    return lax.broadcasted_iota(jnp.int32, shape, dim)


def onehot(cond):
    return jnp.where(cond, 1.0, 0.0).astype(BF16)


def wait_bytes(ref, sem):
    pltpu.make_async_copy(ref, ref, sem).wait()


def kernel(
    og_hbm, gate_hbm, up_hbm, w_hbm, a1_hbm, a2_hbm, plan_hbm,
    gg, gu, ga_ref, gb_ref,
    og, og_ext, gate, up, w, a1, a2, plan,
    slots_out, slots_in, low_out, low_in, low_all,
    chunks, a2_cut, w_cut, thru, acc, c_gate, c_up, hidden_t, earlier,
    b_part, b_out, b_in, b_all, a_out, a_in,
    load_sem, g_recv, sems,
):
    me, mm = lax.axis_index("dp"), lax.axis_index("mp")
    (p_send, p_recv, l_send, l_recv, lg_send, lg_recv, g_send, b_send, b_recv,
     bg_send, bg_recv, r_send, r_recv) = [sems.at[k] for k in range(13)]

    loads = [
        pltpu.make_async_copy(src, dst, load_sem.at[k])
        for k, (src, dst) in enumerate(
            [(plan_hbm, plan), (og_hbm, og), (gate_hbm, gate), (up_hbm, up),
             (a1_hbm, a1), (a2_hbm, a2), (w_hbm, w)]
        )
    ]
    for copy in loads:
        copy.start()

    barrier = pltpu.get_barrier_semaphore()

    @pl.loop(1, DP)
    def _(i):
        pl.semaphore_signal(
            barrier, inc=1, device_id={"dp": lax.rem(me + i, DP)}, device_id_type=MESH
        )

    @pl.loop(1, MP)
    def _(i):
        pl.semaphore_signal(
            barrier, inc=1, device_id={"mp": lax.rem(mm + i, MP)}, device_id_type=MESH
        )

    def give(axis, mine, peer, src, dst, send_sem, recv_sem, by_peer):
        pltpu.make_async_remote_copy(
            src_ref=src.at[peer] if by_peer else src.at[mine],
            dst_ref=dst.at[mine],
            send_sem=send_sem,
            recv_sem=recv_sem,
            device_id={axis: peer},
            device_id_type=MESH,
        ).start()

    def over_mp(src, dst, send_sem, recv_sem, by_peer):
        @pl.loop(1, MP)
        def _(i):
            give("mp", mm, lax.rem(mm + i, MP), src, dst, send_sem, recv_sem, by_peer)

    z = lax.rem(me, NZ)
    base = [lax.rem(me // NZ + e, NY) * NZ for e in range(NY)]

    def over_dp(src, dst, send_sem, recv_sem):
        @pl.loop(0, NZ - 1)
        def _(j):
            step = ((j + 1) >> 1) * (2 * (j & 1) - 1)
            there = lax.rem(z + step + (NZ + NZ // 2), NZ)
            for e in range(NY):
                give("dp", me, base[NY - 1 - e] + there, src, dst, send_sem, recv_sem, True)

        for e in range(1, NY):
            give("dp", me, base[NY - e] + z, src, dst, send_sem, recv_sem, True)

    loads[0].wait()
    expand = onehot(iota((24, TOK), 0) == (iota((24, TOK), 1) >> 3))
    plan_rows = jnp.broadcast_to(plan[...].astype(F32), (8, 24)).astype(BF16)
    owner_of = dot_nn(plan_rows, expand)[0:1, :]
    place = (iota((DP * 8, TOK), 0) >> 3).astype(F32)
    same_row = (iota((DP * 8, TOK), 0) & 7) == (iota((DP * 8, TOK), 1) & 7)
    sending = onehot((owner_of == place) & same_row)
    loads[1].wait()
    og_ext[:, :FEAT] = og[...]
    og_ext[:, FEAT:] = jnp.ones((TOK, WIDE - FEAT), BF16)
    slots_out[...] = dot_nn(sending, og_ext[...]).astype(BF16).reshape(DP, 8, WIDE)
    slots_in[me] = slots_out[me]

    pl.semaphore_wait(barrier, DP - 1 + MP - 1)
    over_dp(slots_out, slots_in, p_send, p_recv)

    loads[2].wait()
    loads[3].wait()
    g = gate[...].astype(F32)
    u = up[...].astype(F32)
    sig = jax.nn.sigmoid(g)
    silu = g * sig
    c_up[...] = silu
    c_gate[...] = u * sig * (1.0 + g * (1.0 - sig))
    hidden = (silu * u).astype(BF16)
    loads[4].wait()
    low_out[...] = jnp.zeros((MP, 16, RW), F32)
    low_out[0 : TOK // 16, :, :RANK] = dot_nt(hidden, a1[...]).reshape(TOK // 16, 16, RANK)
    low_in[mm] = low_out[mm]
    over_mp(low_out, low_in, l_send, l_recv, True)

    row = iota((DP * 16, HID), 0)
    spread = onehot(((row >> 4) * PIECE + (row & 15) == iota((DP * 16, HID), 1)) & ((row & 15) < PIECE))
    hidden_t[...] = dot_nt(spread, hidden).astype(BF16)
    first = iota((DP * 8, DP * 8), 0)
    earlier[...] = onehot(((first >> 3) < (iota((DP * 8, DP * 8), 1) >> 3)) & ((first & 7) == 0))

    loads[5].wait()
    loads[6].wait()
    for k in range(MP):
        cols = slice(k * FEAT, (k + 1) * FEAT)
        a2_cut[k, RANK:, :] = jnp.zeros((RW - RANK, WIDE), BF16)
        a2_cut[k, 0:RANK, FEAT:] = jnp.zeros((RANK, WIDE - FEAT), BF16)
        a2_cut[k, 0:RANK, :FEAT] = a2[:, cols]
        w_cut[k, :, FEAT:] = jnp.zeros((HID, WIDE - FEAT), BF16)
        w_cut[k, :, :FEAT] = w[:, cols]

    wait_bytes(low_in.at[pl.ds(0, MP - 1)], l_recv)
    low_all[mm] = jnp.sum(low_in[...], axis=0).astype(BF16)
    over_mp(low_all, low_all, lg_send, lg_recv, False)

    wait_bytes(slots_in.at[pl.ds(0, DP - 1)], p_recv)
    arrived = slots_in[...].reshape(DP * 8, WIDE)
    pick = onehot(iota((8, WIDE), 1) == FEAT)
    present = dot_nt(pick, arrived)
    rank = dot_nn(present.astype(BF16), earlier[...])
    place = (iota((TOK, DP * 8), 0) >> 3).astype(F32)
    same_row = (iota((TOK, DP * 8), 0) & 7) == (iota((TOK, DP * 8), 1) & 7)
    keeping = onehot((present[0:1, :] > 0.5) & (rank[0:1, :] == place) & same_row)
    packed = dot_nn(keeping, arrived).astype(BF16)
    chunks[mm] = packed

    h, x, c = mm // 8, lax.rem(mm // 2, 4), lax.rem(mm, 2)
    o, s = 1 - h, 1 - c
    ahead = lax.rem(x + 5 - 2 * c, 4)
    behind = lax.rem(x + 3 + 2 * c, 4)
    across = lax.rem(x + 2, 4)

    def at(hh, xx, cc):
        return hh * 8 + xx * 2 + cc

    def send(slot, dest):
        pltpu.make_async_remote_copy(
            src_ref=chunks.at[slot],
            dst_ref=chunks.at[slot],
            send_sem=g_send,
            recv_sem=g_recv.at[slot],
            device_id={"mp": dest},
            device_id_type=MESH,
        ).start()

    def arrive(slot):
        wait_bytes(chunks.at[slot], g_recv.at[slot])

    def consume(slot):
        thru[...] += dot_nt(chunks[slot], a2_cut[slot])

    sibling = at(h, x, s)
    send(mm, at(o, x, c))
    send(mm, at(h, ahead, c))
    send(mm, at(h, behind, c))
    send(mm, sibling)
    thru[...] = dot_nt(packed, a2_cut[mm])

    def second_factor():
        wait_bytes(low_all.at[pl.ds(0, MP - 1)], lg_recv)
        low = low_all[...].reshape(MP * 16, RW)[:TOK, :]
        b_part[...] = dot_tn(low, packed)
        for k in range(DP):
            b_out[k] = b_part[2 * k : 2 * k + 2, :]
        b_in[me] = b_out[me]
        over_dp(b_out, b_in, b_send, b_recv)

    for hh in (h, o):
        if hh is o:
            arrive(at(o, x, c))
            send(at(o, x, c), at(h, ahead, c))
            send(at(o, x, c), at(h, behind, c))
            send(at(o, x, c), sibling)
            consume(at(o, x, c))
        arrive(at(hh, behind, c))
        send(at(hh, behind, c), at(h, ahead, c))
        send(at(hh, behind, c), sibling)
        consume(at(hh, behind, c))
        arrive(at(hh, ahead, c))
        send(at(hh, ahead, c), sibling)
        consume(at(hh, ahead, c))
        if hh is h:
            second_factor()
        arrive(at(hh, across, c))
        send(at(hh, across, c), sibling)
        consume(at(hh, across, c))
        for xx in (x, ahead, behind, across):
            arrive(at(hh, xx, s))
            consume(at(hh, xx, s))

    through = thru[...].astype(BF16)
    a_out[...] = dot_nn(hidden_t[...], through).astype(BF16).reshape(DP, 16, RW)
    a_in[me] = a_out[me]
    over_dp(a_out, a_in, r_send, r_recv)

    wait_bytes(b_in.at[pl.ds(0, DP - 1)], b_recv)
    b_all[mm] = jnp.sum(b_in[...], axis=0)
    over_mp(b_all, b_all, bg_send, bg_recv, False)

    acc[...] = dot_nn(through[:, :RANK], a1[...])

    @pl.loop(0, MP)
    def _(k):
        acc[...] += dot_nt(chunks[k], w_cut[k])

    grad_hidden = acc[...]
    gg[...] = (grad_hidden * c_gate[...]).astype(BF16)
    gu[...] = (grad_hidden * c_up[...]).astype(BF16)

    wait_bytes(b_all.at[pl.ds(0, MP - 1)], bg_recv)
    for k in range(MP):
        gb_ref[:, k * FEAT : (k + 1) * FEAT] = b_all[k][:, :FEAT]

    wait_bytes(slots_out.at[pl.ds(0, DP - 1)], p_send)
    wait_bytes(low_out.at[pl.ds(0, MP - 1)], l_send)
    wait_bytes(low_all.at[pl.ds(0, MP - 1)], lg_send)
    wait_bytes(chunks.at[pl.ds(0, MP - 1)], g_send)
    wait_bytes(b_out.at[pl.ds(0, DP - 1)], b_send)
    wait_bytes(b_all.at[pl.ds(0, MP - 1)], bg_send)
    wait_bytes(a_in.at[pl.ds(0, DP - 1)], r_recv)
    total = jnp.sum(a_in[...].astype(F32), axis=0)
    ga_ref[...] = total[:PIECE, :RANK].reshape(PIECE, 1, RANK)
    wait_bytes(a_out.at[pl.ds(0, DP - 1)], r_send)


def deliver(*refs):
    sources, targets, sem = refs[:4], refs[4:8], refs[8]
    copies = [
        pltpu.make_async_copy(source, target, sem.at[k])
        for k, (source, target) in enumerate(zip(sources, targets))
    ]
    for copy in copies:
        copy.start()
    for copy in copies:
        copy.wait()


def body(og, gate, up, w, a1, a2, plan):
    hbm = pl.BlockSpec(memory_space=pltpu.HBM)
    vmem = pl.BlockSpec(memory_space=pltpu.VMEM)
    V = pltpu.VMEM
    results = (
        jax.ShapeDtypeStruct((TOK, HID), BF16),
        jax.ShapeDtypeStruct((TOK, HID), BF16),
        jax.ShapeDtypeStruct((PIECE, 1, RANK), F32),
        jax.ShapeDtypeStruct((2, MODEL), F32),
    )
    found = pl.pallas_call(
        kernel,
        out_shape=results,
        in_specs=[hbm] * 7,
        out_specs=(vmem,) * 4,
        scratch_shapes=[
            V((TOK, FEAT), BF16),
            V((TOK, WIDE), BF16),
            V((TOK, HID), BF16),
            V((TOK, HID), BF16),
            V((HID, MODEL), BF16),
            V((RANK, HID), BF16),
            V((RANK, MODEL), BF16),
            V((1, 24), jnp.int32),
            V((DP, 8, WIDE), BF16),
            V((DP, 8, WIDE), BF16),
            V((MP, 16, RW), F32),
            V((MP, 16, RW), F32),
            V((MP, 16, RW), BF16),
            V((MP, TOK, WIDE), BF16),
            V((MP, RW, WIDE), BF16),
            V((MP, HID, WIDE), BF16),
            V((TOK, RW), F32),
            V((TOK, HID), F32),
            V((TOK, HID), F32),
            V((TOK, HID), F32),
            V((DP * 16, TOK), BF16),
            V((DP * 8, DP * 8), BF16),
            V((RW, WIDE), F32),
            V((DP, 2, WIDE), F32),
            V((DP, 2, WIDE), F32),
            V((MP, 2, WIDE), F32),
            V((DP, 16, RW), BF16),
            V((DP, 16, RW), BF16),
            pltpu.SemaphoreType.DMA((7,)),
            pltpu.SemaphoreType.DMA((MP,)),
            pltpu.SemaphoreType.DMA((13,)),
        ],
        compiler_params=pltpu.CompilerParams(
            collective_id=0, has_side_effects=True, vmem_limit_bytes=48 * 1024 * 1024
        ),
        name="repack_backward",
    )(*[
        pltpu.with_memory_space_constraint(v, pltpu.HBM)
        for v in (og, gate, up, w, a1.T, a2, plan.reshape(1, 24))
    ])
    gg, gu, ga, gb = pl.pallas_call(
        deliver,
        out_shape=results,
        in_specs=[vmem] * 4,
        out_specs=(hbm,) * 4,
        scratch_shapes=[pltpu.SemaphoreType.DMA((4,))],
        compiler_params=pltpu.CompilerParams(vmem_limit_bytes=1024 * 1024),
        name="deliver",
    )(*found)
    return gg, gu, ga.reshape(1, PIECE, RANK), gb


def solution(mesh):
    return jax.shard_map(
        body,
        mesh=mesh,
        in_specs=(
            P("dp", "mp"),
            P("dp", "mp"),
            P("dp", "mp"),
            P("mp", None),
            P("mp", None),
            P(),
            P("dp"),
        ),
        out_specs=(P("dp", "mp"), P("dp", "mp"), P("mp", "dp", None), P("dp", None)),
        check_vma=False,
    )
```

```python
import jax
import jax.numpy as jnp
from jax import lax
from jax.experimental import pallas as pl
from jax.experimental.pallas import tpu as pltpu
from jax.sharding import PartitionSpec as P

MESH = pl.DeviceIdType.MESH
F32, BF16 = jnp.float32, jnp.bfloat16
DP, MP = 48, 16
TOK, FEAT, WIDE = 192, 224, 256
HID, RANK, RW = 624, 96, 128
PIECE = 13
NY, NZ = 4, 12
MODEL = 3584


def dot_nn(a, b):
    return lax.dot_general(a, b, (((1,), (0,)), ((), ())), preferred_element_type=F32)


def dot_nt(a, b):
    return lax.dot_general(a, b, (((1,), (1,)), ((), ())), preferred_element_type=F32)


def dot_tn(a, b):
    return lax.dot_general(a, b, (((0,), (0,)), ((), ())), preferred_element_type=F32)


def iota(shape, dim):
    return lax.broadcasted_iota(jnp.int32, shape, dim)


def onehot(cond):
    return jnp.where(cond, 1.0, 0.0).astype(BF16)


def wait_bytes(ref, sem):
    pltpu.make_async_copy(ref, ref, sem).wait()


def kernel(
    og_hbm, gate_hbm, up_hbm, w_hbm, a1_hbm, a2_hbm, plan_hbm,
    gg, gu, ga_ref, gb_ref,
    og, og_ext, gate, up, w, a1, a2, plan,
    slots_out, slots_in, low_out, low_in, low_all,
    chunks, a2_cut, w_cut, thru, acc, c_gate, c_up, hidden_t, earlier,
    b_part, b_out, b_in, b_all, a_out, a_in,
    load_sem, g_recv, sems,
):
    me, mm = lax.axis_index("dp"), lax.axis_index("mp")
    (p_send, p_recv, l_send, l_recv, lg_send, lg_recv, g_send, b_send, b_recv,
     bg_send, bg_recv, r_send, r_recv) = [sems.at[k] for k in range(13)]

    loads = [
        pltpu.make_async_copy(src, dst, load_sem.at[k])
        for k, (src, dst) in enumerate(
            [(plan_hbm, plan), (og_hbm, og), (gate_hbm, gate), (up_hbm, up),
             (a1_hbm, a1), (a2_hbm, a2), (w_hbm, w)]
        )
    ]
    for copy in loads:
        copy.start()

    z = lax.rem(me, NZ)
    base = [lax.rem(me // NZ + e, NY) * NZ for e in range(NY)]

    def each_dp(act):
        @pl.loop(0, NZ - 1)
        def _(j):
            step = ((j + 1) >> 1) * (2 * (j & 1) - 1)
            there = lax.rem(z + step + (NZ + NZ // 2), NZ)
            for e in range(NY):
                act(base[NY - 1 - e] + there)

        for e in range(1, NY):
            act(base[NY - e] + z)

    def each_mp(act):
        for k in range(MP - 1):
            off = MP // 2 + (k + 1) // 2 * (1 - 2 * (k % 2))
            act(lax.rem(mm + off, MP))

    barrier = pltpu.get_barrier_semaphore()
    each_dp(lambda peer: pl.semaphore_signal(
        barrier, inc=1, device_id={"dp": peer}, device_id_type=MESH))
    each_mp(lambda peer: pl.semaphore_signal(
        barrier, inc=1, device_id={"mp": peer}, device_id_type=MESH))

    def give(axis, mine, peer, src, dst, send_sem, recv_sem, by_peer):
        pltpu.make_async_remote_copy(
            src_ref=src.at[peer] if by_peer else src.at[mine],
            dst_ref=dst.at[mine],
            send_sem=send_sem,
            recv_sem=recv_sem,
            device_id={axis: peer},
            device_id_type=MESH,
        ).start()

    def over_mp(src, dst, send_sem, recv_sem, by_peer):
        each_mp(lambda peer: give("mp", mm, peer, src, dst, send_sem, recv_sem, by_peer))

    def over_dp(src, dst, send_sem, recv_sem):
        each_dp(lambda peer: give("dp", me, peer, src, dst, send_sem, recv_sem, True))

    loads[0].wait()
    expand = onehot(iota((24, TOK), 0) == (iota((24, TOK), 1) >> 3))
    plan_rows = jnp.broadcast_to(plan[...].astype(F32), (8, 24)).astype(BF16)
    owner_of = dot_nn(plan_rows, expand)[0:1, :]
    place = (iota((DP * 8, TOK), 0) >> 3).astype(F32)
    same_row = (iota((DP * 8, TOK), 0) & 7) == (iota((DP * 8, TOK), 1) & 7)
    sending = onehot((owner_of == place) & same_row)
    loads[1].wait()
    og_ext[:, :FEAT] = og[...]
    og_ext[:, FEAT:] = jnp.ones((TOK, WIDE - FEAT), BF16)
    slots_out[...] = dot_nn(sending, og_ext[...]).astype(BF16).reshape(DP, 8, WIDE)
    slots_in[me] = slots_out[me]

    pl.semaphore_wait(barrier, DP - 1 + MP - 1)
    over_dp(slots_out, slots_in, p_send, p_recv)

    loads[2].wait()
    loads[3].wait()
    g = gate[...].astype(F32)
    u = up[...].astype(F32)
    sig = jax.nn.sigmoid(g)
    silu = g * sig
    c_up[...] = silu
    c_gate[...] = u * sig * (1.0 + g * (1.0 - sig))
    hidden = (silu * u).astype(BF16)
    loads[4].wait()
    low_out[...] = jnp.zeros((MP, 16, RW), F32)
    low_out[0 : TOK // 16, :, :RANK] = dot_nt(hidden, a1[...]).reshape(TOK // 16, 16, RANK)
    low_in[mm] = low_out[mm]
    over_mp(low_out, low_in, l_send, l_recv, True)

    row = iota((DP * 16, HID), 0)
    spread = onehot(((row >> 4) * PIECE + (row & 15) == iota((DP * 16, HID), 1)) & ((row & 15) < PIECE))
    hidden_t[...] = dot_nt(spread, hidden).astype(BF16)
    first = iota((DP * 8, DP * 8), 0)
    earlier[...] = onehot(((first >> 3) < (iota((DP * 8, DP * 8), 1) >> 3)) & ((first & 7) == 0))

    loads[5].wait()
    loads[6].wait()
    for k in range(MP):
        cols = slice(k * FEAT, (k + 1) * FEAT)
        a2_cut[k, RANK:, :] = jnp.zeros((RW - RANK, WIDE), BF16)
        a2_cut[k, 0:RANK, FEAT:] = jnp.zeros((RANK, WIDE - FEAT), BF16)
        a2_cut[k, 0:RANK, :FEAT] = a2[:, cols]
        w_cut[k, :, FEAT:] = jnp.zeros((HID, WIDE - FEAT), BF16)
        w_cut[k, :, :FEAT] = w[:, cols]

    wait_bytes(low_in.at[pl.ds(0, MP - 1)], l_recv)
    low_all[mm] = jnp.sum(low_in[...], axis=0).astype(BF16)
    over_mp(low_all, low_all, lg_send, lg_recv, False)

    wait_bytes(slots_in.at[pl.ds(0, DP - 1)], p_recv)
    arrived = slots_in[...].reshape(DP * 8, WIDE)
    pick = onehot(iota((8, WIDE), 1) == FEAT)
    present = dot_nt(pick, arrived)
    rank = dot_nn(present.astype(BF16), earlier[...])
    place = (iota((TOK, DP * 8), 0) >> 3).astype(F32)
    same_row = (iota((TOK, DP * 8), 0) & 7) == (iota((TOK, DP * 8), 1) & 7)
    keeping = onehot((present[0:1, :] > 0.5) & (rank[0:1, :] == place) & same_row)
    packed = dot_nn(keeping, arrived).astype(BF16)
    chunks[mm] = packed.reshape(2, TOK // 2, WIDE)

    h, x, c = mm // 8, lax.rem(mm // 2, 4), lax.rem(mm, 2)
    o, s = 1 - h, 1 - c
    ahead = lax.rem(x + 5 - 2 * c, 4)
    behind = lax.rem(x + 3 + 2 * c, 4)
    across = lax.rem(x + 2, 4)

    def at(hh, xx, cc):
        return hh * 8 + xx * 2 + cc

    def send(slot, half, *dests):
        for dest in dests:
            pltpu.make_async_remote_copy(
                src_ref=chunks.at[slot, half],
                dst_ref=chunks.at[slot, half],
                send_sem=g_send,
                recv_sem=g_recv.at[slot, half],
                device_id={"mp": dest},
                device_id_type=MESH,
            ).start()

    def arrive(slot, half):
        wait_bytes(chunks.at[slot, half], g_recv.at[slot, half])

    def whole(slot):
        return chunks[slot].reshape(TOK, WIDE)

    def consume(slot):
        thru[...] += dot_nt(whole(slot), a2_cut[slot])

    sibling = at(h, x, s)
    fore, back = at(h, ahead, c), at(h, behind, c)
    for half in (0, 1):
        send(mm, half, at(o, x, c))
    for half in (0, 1):
        send(mm, half, fore, back)
    for half in (0, 1):
        send(mm, half, sibling)
    thru[...] = dot_nt(packed, a2_cut[mm])

    def second_factor():
        wait_bytes(low_all.at[pl.ds(0, MP - 1)], lg_recv)
        low = low_all[...].reshape(MP * 16, RW)[:TOK, :]
        b_part[...] = dot_tn(low, packed)
        for k in range(DP):
            b_out[k] = b_part[2 * k : 2 * k + 2, :]
        b_in[me] = b_out[me]
        over_dp(b_out, b_in, b_send, b_recv)

    def neighbours(hh):
        for half in (0, 1):
            arrive(at(hh, behind, c), half)
            send(at(hh, behind, c), half, fore, sibling)
        for half in (0, 1):
            arrive(at(hh, ahead, c), half)
            send(at(hh, ahead, c), half, sibling)

    def last(hh, half):
        arrive(at(hh, across, c), half)
        send(at(hh, across, c), half, sibling)

    def add(hh):
        for xx in (behind, ahead, across):
            consume(at(hh, xx, c))
        for xx in (x, ahead, behind, across):
            for half in (0, 1):
                arrive(at(hh, xx, s), half)
            consume(at(hh, xx, s))

    neighbours(h)
    for half in (0, 1):
        arrive(at(o, x, c), half)
        send(at(o, x, c), half, fore, back, sibling)
        last(h, half)
    second_factor()
    consume(at(o, x, c))
    add(h)
    neighbours(o)
    for half in (0, 1):
        last(o, half)
    add(o)

    through = thru[...].astype(BF16)
    a_out[...] = dot_nn(hidden_t[...], through).astype(BF16).reshape(DP, 16, RW)
    a_in[me] = a_out[me]
    over_dp(a_out, a_in, r_send, r_recv)

    wait_bytes(b_in.at[pl.ds(0, DP - 1)], b_recv)
    b_all[mm] = jnp.sum(b_in[...], axis=0)
    over_mp(b_all, b_all, bg_send, bg_recv, False)

    acc[...] = dot_nn(through[:, :RANK], a1[...])

    @pl.loop(0, MP)
    def _(k):
        acc[...] += dot_nt(whole(k), w_cut[k])

    grad_hidden = acc[...]
    gg[...] = (grad_hidden * c_gate[...]).astype(BF16)
    gu[...] = (grad_hidden * c_up[...]).astype(BF16)

    wait_bytes(b_all.at[pl.ds(0, MP - 1)], bg_recv)
    for k in range(MP):
        gb_ref[:, k * FEAT : (k + 1) * FEAT] = b_all[k][:, :FEAT]

    wait_bytes(slots_out.at[pl.ds(0, DP - 1)], p_send)
    wait_bytes(low_out.at[pl.ds(0, MP - 1)], l_send)
    wait_bytes(low_all.at[pl.ds(0, MP - 1)], lg_send)
    wait_bytes(chunks.at[pl.ds(0, MP - 1)], g_send)
    wait_bytes(b_out.at[pl.ds(0, DP - 1)], b_send)
    wait_bytes(b_all.at[pl.ds(0, MP - 1)], bg_send)
    wait_bytes(a_in.at[pl.ds(0, DP - 1)], r_recv)
    total = jnp.sum(a_in[...].astype(F32), axis=0)
    ga_ref[...] = total[:PIECE, :RANK].reshape(PIECE, 1, RANK)
    wait_bytes(a_out.at[pl.ds(0, DP - 1)], r_send)


def deliver(*refs):
    sources, targets, sem = refs[:4], refs[4:8], refs[8]
    copies = [
        pltpu.make_async_copy(source, target, sem.at[k])
        for k, (source, target) in enumerate(zip(sources, targets))
    ]
    for copy in copies:
        copy.start()
    for copy in copies:
        copy.wait()


def body(og, gate, up, w, a1, a2, plan):
    hbm = pl.BlockSpec(memory_space=pltpu.HBM)
    vmem = pl.BlockSpec(memory_space=pltpu.VMEM)
    V = pltpu.VMEM
    results = (
        jax.ShapeDtypeStruct((TOK, HID), BF16),
        jax.ShapeDtypeStruct((TOK, HID), BF16),
        jax.ShapeDtypeStruct((PIECE, 1, RANK), F32),
        jax.ShapeDtypeStruct((2, MODEL), F32),
    )
    found = pl.pallas_call(
        kernel,
        out_shape=results,
        in_specs=[hbm] * 7,
        out_specs=(vmem,) * 4,
        scratch_shapes=[
            V((TOK, FEAT), BF16),
            V((TOK, WIDE), BF16),
            V((TOK, HID), BF16),
            V((TOK, HID), BF16),
            V((HID, MODEL), BF16),
            V((RANK, HID), BF16),
            V((RANK, MODEL), BF16),
            V((1, 24), jnp.int32),
            V((DP, 8, WIDE), BF16),
            V((DP, 8, WIDE), BF16),
            V((MP, 16, RW), F32),
            V((MP, 16, RW), F32),
            V((MP, 16, RW), BF16),
            V((MP, 2, TOK // 2, WIDE), BF16),
            V((MP, RW, WIDE), BF16),
            V((MP, HID, WIDE), BF16),
            V((TOK, RW), F32),
            V((TOK, HID), F32),
            V((TOK, HID), F32),
            V((TOK, HID), F32),
            V((DP * 16, TOK), BF16),
            V((DP * 8, DP * 8), BF16),
            V((RW, WIDE), F32),
            V((DP, 2, WIDE), F32),
            V((DP, 2, WIDE), F32),
            V((MP, 2, WIDE), F32),
            V((DP, 16, RW), BF16),
            V((DP, 16, RW), BF16),
            pltpu.SemaphoreType.DMA((7,)),
            pltpu.SemaphoreType.DMA((MP, 2)),
            pltpu.SemaphoreType.DMA((13,)),
        ],
        compiler_params=pltpu.CompilerParams(
            collective_id=0, has_side_effects=True, vmem_limit_bytes=48 * 1024 * 1024
        ),
        name="repack_backward",
    )(*[
        pltpu.with_memory_space_constraint(v, pltpu.HBM)
        for v in (og, gate, up, w, a1.T, a2, plan.reshape(1, 24))
    ])
    gg, gu, ga, gb = pl.pallas_call(
        deliver,
        out_shape=results,
        in_specs=[vmem] * 4,
        out_specs=(hbm,) * 4,
        scratch_shapes=[pltpu.SemaphoreType.DMA((4,))],
        compiler_params=pltpu.CompilerParams(vmem_limit_bytes=1024 * 1024),
        name="deliver",
    )(*found)
    return gg, gu, ga.reshape(1, PIECE, RANK), gb


def solution(mesh):
    return jax.shard_map(
        body,
        mesh=mesh,
        in_specs=(
            P("dp", "mp"),
            P("dp", "mp"),
            P("dp", "mp"),
            P("mp", None),
            P("mp", None),
            P(),
            P("dp"),
        ),
        out_specs=(P("dp", "mp"), P("dp", "mp"), P("mp", "dp", None), P("dp", None)),
        check_vma=False,
    )
```

```python
import jax
import jax.numpy as jnp
from jax import lax
from jax.experimental import pallas as pl
from jax.experimental.pallas import tpu as pltpu
from jax.sharding import PartitionSpec as P

MESH = pl.DeviceIdType.MESH
F32, BF16 = jnp.float32, jnp.bfloat16
DP, MP = 48, 16
TOK, FEAT, WIDE = 192, 224, 256
HID, RANK, RW = 624, 96, 128
PIECE = 13
NY, NZ = 4, 12
MODEL = 3584


def dot_nn(a, b):
    return lax.dot_general(a, b, (((1,), (0,)), ((), ())), preferred_element_type=F32)


def dot_nt(a, b):
    return lax.dot_general(a, b, (((1,), (1,)), ((), ())), preferred_element_type=F32)


def dot_tn(a, b):
    return lax.dot_general(a, b, (((0,), (0,)), ((), ())), preferred_element_type=F32)


def iota(shape, dim):
    return lax.broadcasted_iota(jnp.int32, shape, dim)


def onehot(cond):
    return jnp.where(cond, 1.0, 0.0).astype(BF16)


def wait_bytes(ref, sem):
    pltpu.make_async_copy(ref, ref, sem).wait()


def kernel(
    og_hbm, gate_hbm, up_hbm, w_hbm, a1_hbm, a2_hbm, plan_hbm,
    gg, gu, ga_ref, gb_ref,
    og, og_ext, gate, up, w, a1, a2, plan,
    slots_out, slots_in, low_out, low_in, low_all,
    chunks, a2_cut, w_cut, thru, acc, c_gate, c_up, hidden_t, earlier,
    b_part, b_out, b_in, b_all, a_out, a_in,
    load_sem, g_recv, sems,
):
    me, mm = lax.axis_index("dp"), lax.axis_index("mp")
    (p_send, p_recv, l_send, l_recv, lg_send, lg_recv, g_send, b_send, b_recv,
     bg_send, bg_recv, r_send, r_recv) = [sems.at[k] for k in range(13)]

    loads = [
        pltpu.make_async_copy(src, dst, load_sem.at[k])
        for k, (src, dst) in enumerate(
            [(plan_hbm, plan), (og_hbm, og), (gate_hbm, gate), (up_hbm, up),
             (a1_hbm, a1), (a2_hbm, a2), (w_hbm, w)]
        )
    ]
    for copy in loads[:2]:
        copy.start()

    z = lax.rem(me, NZ)
    base = [lax.rem(me // NZ + e, NY) * NZ for e in range(NY)]

    def each_dp(act):
        @pl.loop(0, NZ - 1)
        def _(j):
            step = ((j + 1) >> 1) * (2 * (j & 1) - 1)
            there = lax.rem(z + step + (NZ + NZ // 2), NZ)
            for e in range(NY):
                act(base[NY - 1 - e] + there)

        for e in range(1, NY):
            act(base[NY - e] + z)

    def each_mp(act):
        for k in range(MP - 1):
            off = MP // 2 + (k + 1) // 2 * (1 - 2 * (k % 2))
            act(lax.rem(mm + off, MP))

    barrier = pltpu.get_barrier_semaphore()
    each_dp(lambda peer: pl.semaphore_signal(
        barrier, inc=1, device_id={"dp": peer}, device_id_type=MESH))
    each_mp(lambda peer: pl.semaphore_signal(
        barrier, inc=1, device_id={"mp": peer}, device_id_type=MESH))
    for copy in loads[2:]:
        copy.start()

    def give(axis, mine, peer, src, dst, send_sem, recv_sem, by_peer):
        pltpu.make_async_remote_copy(
            src_ref=src.at[peer] if by_peer else src.at[mine],
            dst_ref=dst.at[mine],
            send_sem=send_sem,
            recv_sem=recv_sem,
            device_id={axis: peer},
            device_id_type=MESH,
        ).start()

    def over_mp(src, dst, send_sem, recv_sem, by_peer):
        each_mp(lambda peer: give("mp", mm, peer, src, dst, send_sem, recv_sem, by_peer))

    def over_dp(src, dst, send_sem, recv_sem):
        each_dp(lambda peer: give("dp", me, peer, src, dst, send_sem, recv_sem, True))

    loads[0].wait()
    expand = onehot(iota((24, TOK), 0) == (iota((24, TOK), 1) >> 3))
    plan_rows = jnp.broadcast_to(plan[...].astype(F32), (8, 24)).astype(BF16)
    owner_of = dot_nn(plan_rows, expand)[0:1, :]
    place = (iota((DP * 8, TOK), 0) >> 3).astype(F32)
    same_row = (iota((DP * 8, TOK), 0) & 7) == (iota((DP * 8, TOK), 1) & 7)
    sending = onehot((owner_of == place) & same_row)
    loads[1].wait()
    og_ext[:, :FEAT] = og[...]
    og_ext[:, FEAT:] = jnp.ones((TOK, WIDE - FEAT), BF16)
    slots_out[...] = dot_nn(sending, og_ext[...]).astype(BF16).reshape(DP, 8, WIDE)
    slots_in[me] = slots_out[me]

    loads[2].wait()
    loads[3].wait()
    g = gate[...].astype(F32)
    u = up[...].astype(F32)
    sig = jax.nn.sigmoid(g)
    silu = g * sig
    c_up[...] = silu
    c_gate[...] = u * sig * (1.0 + g * (1.0 - sig))
    hidden = (silu * u).astype(BF16)
    loads[4].wait()
    low_out[...] = jnp.zeros((MP, 16, RW), BF16)
    low_part = dot_nt(hidden, a1[...]).astype(BF16)
    low_out[0 : TOK // 16, :, :RANK] = low_part.reshape(TOK // 16, 16, RANK)
    low_in[mm] = low_out[mm]

    pl.semaphore_wait(barrier, DP - 1 + MP - 1)
    over_dp(slots_out, slots_in, p_send, p_recv)
    over_mp(low_out, low_in, l_send, l_recv, True)

    row = iota((DP * 16, HID), 0)
    spread = onehot(((row >> 4) * PIECE + (row & 15) == iota((DP * 16, HID), 1)) & ((row & 15) < PIECE))
    hidden_t[...] = dot_nt(spread, hidden).astype(BF16)
    first = iota((DP * 8, DP * 8), 0)
    earlier[...] = onehot(((first >> 3) < (iota((DP * 8, DP * 8), 1) >> 3)) & ((first & 7) == 0))

    loads[5].wait()
    loads[6].wait()
    for k in range(MP):
        cols = slice(k * FEAT, (k + 1) * FEAT)
        a2_cut[k, RANK:, :] = jnp.zeros((RW - RANK, WIDE), BF16)
        a2_cut[k, 0:RANK, FEAT:] = jnp.zeros((RANK, WIDE - FEAT), BF16)
        a2_cut[k, 0:RANK, :FEAT] = a2[:, cols]
        w_cut[k, :, FEAT:] = jnp.zeros((HID, WIDE - FEAT), BF16)
        w_cut[k, :, :FEAT] = w[:, cols]

    wait_bytes(low_in.at[pl.ds(0, MP - 1)], l_recv)
    low_all[mm] = jnp.sum(low_in[...].astype(F32), axis=0).astype(BF16)
    over_mp(low_all, low_all, lg_send, lg_recv, False)

    wait_bytes(slots_in.at[pl.ds(0, DP - 1)], p_recv)
    arrived = slots_in[...].reshape(DP * 8, WIDE)
    pick = onehot(iota((8, WIDE), 1) == FEAT)
    present = dot_nt(pick, arrived)
    rank = dot_nn(present.astype(BF16), earlier[...])
    place = (iota((TOK, DP * 8), 0) >> 3).astype(F32)
    same_row = (iota((TOK, DP * 8), 0) & 7) == (iota((TOK, DP * 8), 1) & 7)
    keeping = onehot((present[0:1, :] > 0.5) & (rank[0:1, :] == place) & same_row)
    packed = dot_nn(keeping, arrived).astype(BF16)
    chunks[mm] = packed.reshape(2, TOK // 2, WIDE)

    h, x, c = mm // 8, lax.rem(mm // 2, 4), lax.rem(mm, 2)
    o, s = 1 - h, 1 - c
    ahead = lax.rem(x + 5 - 2 * c, 4)
    behind = lax.rem(x + 3 + 2 * c, 4)
    across = lax.rem(x + 2, 4)

    def at(hh, xx, cc):
        return hh * 8 + xx * 2 + cc

    def send(slot, half, *dests):
        for dest in dests:
            pltpu.make_async_remote_copy(
                src_ref=chunks.at[slot, half],
                dst_ref=chunks.at[slot, half],
                send_sem=g_send,
                recv_sem=g_recv.at[slot, half],
                device_id={"mp": dest},
                device_id_type=MESH,
            ).start()

    def arrive(slot, half):
        wait_bytes(chunks.at[slot, half], g_recv.at[slot, half])

    def whole(slot):
        return chunks[slot].reshape(TOK, WIDE)

    def consume(slot):
        thru[...] += dot_nt(whole(slot), a2_cut[slot])

    sibling = at(h, x, s)
    fore, back = at(h, ahead, c), at(h, behind, c)
    for half in (0, 1):
        send(mm, half, at(o, x, c))
    for half in (0, 1):
        send(mm, half, fore, back)
    for half in (0, 1):
        send(mm, half, sibling)
    thru[...] = dot_nt(packed, a2_cut[mm])

    def second_factor():
        wait_bytes(low_all.at[pl.ds(0, MP - 1)], lg_recv)
        low = low_all[...].reshape(MP * 16, RW)[:TOK, :]
        b_part[...] = dot_tn(low, packed)
        for k in range(DP):
            b_out[k] = b_part[2 * k : 2 * k + 2, :]
        b_in[me] = b_out[me]
        over_dp(b_out, b_in, b_send, b_recv)

    def neighbours(hh):
        for half in (0, 1):
            arrive(at(hh, behind, c), half)
            send(at(hh, behind, c), half, fore, sibling)
        for half in (0, 1):
            arrive(at(hh, ahead, c), half)
            send(at(hh, ahead, c), half, sibling)

    def last(hh, half):
        arrive(at(hh, across, c), half)
        send(at(hh, across, c), half, sibling)

    def add(hh):
        for xx in (behind, ahead, across):
            consume(at(hh, xx, c))
        for xx in (x, ahead, behind, across):
            for half in (0, 1):
                arrive(at(hh, xx, s), half)
            consume(at(hh, xx, s))

    neighbours(h)
    for half in (0, 1):
        arrive(at(o, x, c), half)
        send(at(o, x, c), half, fore, back, sibling)
        last(h, half)
    second_factor()
    neighbours(o)
    consume(at(o, x, c))
    add(h)
    for half in (0, 1):
        last(o, half)
    add(o)

    through = thru[...].astype(BF16)
    a_out[...] = dot_nn(hidden_t[...], through).astype(BF16).reshape(DP, 16, RW)
    a_in[me] = a_out[me]
    over_dp(a_out, a_in, r_send, r_recv)

    wait_bytes(b_in.at[pl.ds(0, DP - 1)], b_recv)
    b_all[mm] = jnp.sum(b_in[...], axis=0)
    over_mp(b_all, b_all, bg_send, bg_recv, False)

    acc[...] = dot_nn(through[:, :RANK], a1[...])

    @pl.loop(0, MP)
    def _(k):
        acc[...] += dot_nt(whole(k), w_cut[k])

    grad_hidden = acc[...]
    gg[...] = (grad_hidden * c_gate[...]).astype(BF16)
    gu[...] = (grad_hidden * c_up[...]).astype(BF16)

    wait_bytes(b_all.at[pl.ds(0, MP - 1)], bg_recv)
    for k in range(MP):
        gb_ref[:, k * FEAT : (k + 1) * FEAT] = b_all[k][:, :FEAT]

    wait_bytes(slots_out.at[pl.ds(0, DP - 1)], p_send)
    wait_bytes(low_out.at[pl.ds(0, MP - 1)], l_send)
    wait_bytes(low_all.at[pl.ds(0, MP - 1)], lg_send)
    wait_bytes(chunks.at[pl.ds(0, MP - 1)], g_send)
    wait_bytes(b_out.at[pl.ds(0, DP - 1)], b_send)
    wait_bytes(b_all.at[pl.ds(0, MP - 1)], bg_send)
    wait_bytes(a_in.at[pl.ds(0, DP - 1)], r_recv)
    total = jnp.sum(a_in[...].astype(F32), axis=0)
    ga_ref[...] = total[:PIECE, :RANK].reshape(PIECE, 1, RANK)
    wait_bytes(a_out.at[pl.ds(0, DP - 1)], r_send)


def deliver(*refs):
    sources, targets, sem = refs[:4], refs[4:8], refs[8]
    copies = [
        pltpu.make_async_copy(source, target, sem.at[k])
        for k, (source, target) in enumerate(zip(sources, targets))
    ]
    for copy in copies:
        copy.start()
    for copy in copies:
        copy.wait()


def body(og, gate, up, w, a1, a2, plan):
    hbm = pl.BlockSpec(memory_space=pltpu.HBM)
    vmem = pl.BlockSpec(memory_space=pltpu.VMEM)
    V = pltpu.VMEM
    results = (
        jax.ShapeDtypeStruct((TOK, HID), BF16),
        jax.ShapeDtypeStruct((TOK, HID), BF16),
        jax.ShapeDtypeStruct((PIECE, 1, RANK), F32),
        jax.ShapeDtypeStruct((2, MODEL), F32),
    )
    found = pl.pallas_call(
        kernel,
        out_shape=results,
        in_specs=[hbm] * 7,
        out_specs=(vmem,) * 4,
        scratch_shapes=[
            V((TOK, FEAT), BF16),
            V((TOK, WIDE), BF16),
            V((TOK, HID), BF16),
            V((TOK, HID), BF16),
            V((HID, MODEL), BF16),
            V((RANK, HID), BF16),
            V((RANK, MODEL), BF16),
            V((1, 24), jnp.int32),
            V((DP, 8, WIDE), BF16),
            V((DP, 8, WIDE), BF16),
            V((MP, 16, RW), BF16),
            V((MP, 16, RW), BF16),
            V((MP, 16, RW), BF16),
            V((MP, 2, TOK // 2, WIDE), BF16),
            V((MP, RW, WIDE), BF16),
            V((MP, HID, WIDE), BF16),
            V((TOK, RW), F32),
            V((TOK, HID), F32),
            V((TOK, HID), F32),
            V((TOK, HID), F32),
            V((DP * 16, TOK), BF16),
            V((DP * 8, DP * 8), BF16),
            V((RW, WIDE), F32),
            V((DP, 2, WIDE), F32),
            V((DP, 2, WIDE), F32),
            V((MP, 2, WIDE), F32),
            V((DP, 16, RW), BF16),
            V((DP, 16, RW), BF16),
            pltpu.SemaphoreType.DMA((7,)),
            pltpu.SemaphoreType.DMA((MP, 2)),
            pltpu.SemaphoreType.DMA((13,)),
        ],
        compiler_params=pltpu.CompilerParams(
            collective_id=0, has_side_effects=True, vmem_limit_bytes=48 * 1024 * 1024
        ),
        name="repack_backward",
    )(*[
        pltpu.with_memory_space_constraint(v, pltpu.HBM)
        for v in (og, gate, up, w, a1.T, a2, plan.reshape(1, 24))
    ])
    gg, gu, ga, gb = pl.pallas_call(
        deliver,
        out_shape=results,
        in_specs=[vmem] * 4,
        out_specs=(hbm,) * 4,
        scratch_shapes=[pltpu.SemaphoreType.DMA((4,))],
        compiler_params=pltpu.CompilerParams(vmem_limit_bytes=1024 * 1024),
        name="deliver",
    )(*found)
    return gg, gu, ga.reshape(1, PIECE, RANK), gb


def solution(mesh):
    return jax.shard_map(
        body,
        mesh=mesh,
        in_specs=(
            P("dp", "mp"),
            P("dp", "mp"),
            P("dp", "mp"),
            P("mp", None),
            P("mp", None),
            P(),
            P("dp"),
        ),
        out_specs=(P("dp", "mp"), P("dp", "mp"), P("mp", "dp", None), P("dp", None)),
        check_vma=False,
    )
```

```python
import jax
import jax.numpy as jnp
from jax import lax
from jax.experimental import pallas as pl
from jax.experimental.pallas import tpu as pltpu
from jax.sharding import PartitionSpec as P

MESH = pl.DeviceIdType.MESH
F32, BF16 = jnp.float32, jnp.bfloat16
DP, MP = 48, 16
TOK, FEAT, WIDE = 192, 224, 256
HID, RANK, RW = 624, 96, 128
PIECE = 13
NY, NZ = 4, 12
PARTS = 3
MODEL = 3584


def dot_nn(a, b):
    return lax.dot_general(a, b, (((1,), (0,)), ((), ())), preferred_element_type=F32)


def dot_nt(a, b):
    return lax.dot_general(a, b, (((1,), (1,)), ((), ())), preferred_element_type=F32)


def dot_tn(a, b):
    return lax.dot_general(a, b, (((0,), (0,)), ((), ())), preferred_element_type=F32)


def iota(shape, dim):
    return lax.broadcasted_iota(jnp.int32, shape, dim)


def onehot(cond):
    return jnp.where(cond, 1.0, 0.0).astype(BF16)


def wait_bytes(ref, sem):
    pltpu.make_async_copy(ref, ref, sem).wait()


def kernel(
    og_hbm, gate_hbm, up_hbm, w_hbm, a1_hbm, a2_hbm, plan_hbm,
    gg, gu, ga_ref, gb_ref,
    og, og_ext, gate, up, w, a1, a2, plan,
    slots_out, slots_in, low_out, low_in, low_all,
    chunks, a2_cut, w_cut, thru, acc, c_gate, c_up, hidden_t, earlier,
    b_part, b_out, b_in, b_all, a_out, a_in,
    load_sem, g_recv, sems,
):
    me, mm = lax.axis_index("dp"), lax.axis_index("mp")
    (p_send, p_recv, l_send, l_recv, lg_send, lg_recv, g_send, b_send, b_recv,
     bg_send, bg_recv, r_send, r_recv) = [sems.at[k] for k in range(13)]

    loads = [
        pltpu.make_async_copy(src, dst, load_sem.at[k])
        for k, (src, dst) in enumerate(
            [(plan_hbm, plan), (og_hbm, og), (gate_hbm, gate), (up_hbm, up),
             (a1_hbm, a1), (a2_hbm, a2), (w_hbm, w)]
        )
    ]
    for copy in loads[:2]:
        copy.start()

    z = lax.rem(me, NZ)
    base = [lax.rem(me // NZ + e, NY) * NZ for e in range(NY)]

    def each_dp(act):
        @pl.loop(0, NZ - 1)
        def _(j):
            step = ((j + 1) >> 1) * (2 * (j & 1) - 1)
            there = lax.rem(z + step + (NZ + NZ // 2), NZ)
            for e in range(NY):
                act(base[NY - 1 - e] + there)

        for e in range(1, NY):
            act(base[NY - e] + z)

    def each_mp(act):
        for k in range(MP - 1):
            off = MP // 2 + (k + 1) // 2 * (1 - 2 * (k % 2))
            act(lax.rem(mm + off, MP))

    barrier = pltpu.get_barrier_semaphore()
    each_dp(lambda peer: pl.semaphore_signal(
        barrier, inc=1, device_id={"dp": peer}, device_id_type=MESH))
    each_mp(lambda peer: pl.semaphore_signal(
        barrier, inc=1, device_id={"mp": peer}, device_id_type=MESH))
    for copy in loads[2:]:
        copy.start()

    def give(axis, mine, peer, src, dst, send_sem, recv_sem, by_peer):
        pltpu.make_async_remote_copy(
            src_ref=src.at[peer] if by_peer else src.at[mine],
            dst_ref=dst.at[mine],
            send_sem=send_sem,
            recv_sem=recv_sem,
            device_id={axis: peer},
            device_id_type=MESH,
        ).start()

    def over_mp(src, dst, send_sem, recv_sem, by_peer):
        each_mp(lambda peer: give("mp", mm, peer, src, dst, send_sem, recv_sem, by_peer))

    def over_dp(src, dst, send_sem, recv_sem):
        each_dp(lambda peer: give("dp", me, peer, src, dst, send_sem, recv_sem, True))

    loads[0].wait()
    expand = onehot(iota((24, TOK), 0) == (iota((24, TOK), 1) >> 3))
    plan_rows = jnp.broadcast_to(plan[...].astype(F32), (8, 24)).astype(BF16)
    owner_of = dot_nn(plan_rows, expand)[0:1, :]
    place = (iota((DP * 8, TOK), 0) >> 3).astype(F32)
    same_row = (iota((DP * 8, TOK), 0) & 7) == (iota((DP * 8, TOK), 1) & 7)
    sending = onehot((owner_of == place) & same_row)
    loads[1].wait()
    og_ext[:, :FEAT] = og[...]
    og_ext[:, FEAT:] = jnp.ones((TOK, WIDE - FEAT), BF16)
    slots_out[...] = dot_nn(sending, og_ext[...]).astype(BF16).reshape(DP, 8, WIDE)
    slots_in[me] = slots_out[me]

    loads[2].wait()
    loads[3].wait()
    g = gate[...].astype(F32)
    u = up[...].astype(F32)
    sig = jax.nn.sigmoid(g)
    silu = g * sig
    c_up[...] = silu
    c_gate[...] = u * sig * (1.0 + g * (1.0 - sig))
    hidden = (silu * u).astype(BF16)
    loads[4].wait()
    low_out[...] = jnp.zeros((MP, 16, RW), BF16)
    low_part = dot_nt(hidden, a1[...]).astype(BF16)
    low_out[0 : TOK // 16, :, :RANK] = low_part.reshape(TOK // 16, 16, RANK)
    low_in[mm] = low_out[mm]

    pl.semaphore_wait(barrier, DP - 1 + MP - 1)
    over_dp(slots_out, slots_in, p_send, p_recv)
    over_mp(low_out, low_in, l_send, l_recv, True)

    row = iota((DP * 16, HID), 0)
    spread = onehot(((row >> 4) * PIECE + (row & 15) == iota((DP * 16, HID), 1)) & ((row & 15) < PIECE))
    hidden_t[...] = dot_nt(spread, hidden).astype(BF16)
    first = iota((DP * 8, DP * 8), 0)
    earlier[...] = onehot(((first >> 3) < (iota((DP * 8, DP * 8), 1) >> 3)) & ((first & 7) == 0))

    loads[5].wait()
    loads[6].wait()
    for k in range(MP):
        cols = slice(k * FEAT, (k + 1) * FEAT)
        a2_cut[k, RANK:, :] = jnp.zeros((RW - RANK, WIDE), BF16)
        a2_cut[k, 0:RANK, FEAT:] = jnp.zeros((RANK, WIDE - FEAT), BF16)
        a2_cut[k, 0:RANK, :FEAT] = a2[:, cols]
        w_cut[k, :, FEAT:] = jnp.zeros((HID, WIDE - FEAT), BF16)
        w_cut[k, :, :FEAT] = w[:, cols]

    wait_bytes(low_in.at[pl.ds(0, MP - 1)], l_recv)
    low_all[mm] = jnp.sum(low_in[...].astype(F32), axis=0).astype(BF16)
    over_mp(low_all, low_all, lg_send, lg_recv, False)

    wait_bytes(slots_in.at[pl.ds(0, DP - 1)], p_recv)
    arrived = slots_in[...].reshape(DP * 8, WIDE)
    pick = onehot(iota((8, WIDE), 1) == FEAT)
    present = dot_nt(pick, arrived)
    rank = dot_nn(present.astype(BF16), earlier[...])
    place = (iota((TOK, DP * 8), 0) >> 3).astype(F32)
    same_row = (iota((TOK, DP * 8), 0) & 7) == (iota((TOK, DP * 8), 1) & 7)
    keeping = onehot((present[0:1, :] > 0.5) & (rank[0:1, :] == place) & same_row)
    packed = dot_nn(keeping, arrived).astype(BF16)
    chunks[mm] = packed.reshape(PARTS, TOK // PARTS, WIDE)

    h, x, c = mm // 8, lax.rem(mm // 2, 4), lax.rem(mm, 2)
    o, s = 1 - h, 1 - c
    ahead = lax.rem(x + 5 - 2 * c, 4)
    behind = lax.rem(x + 3 + 2 * c, 4)
    across = lax.rem(x + 2, 4)

    def at(hh, xx, cc):
        return hh * 8 + xx * 2 + cc

    def send(slot, part, *dests):
        for dest in dests:
            pltpu.make_async_remote_copy(
                src_ref=chunks.at[slot, part],
                dst_ref=chunks.at[slot, part],
                send_sem=g_send,
                recv_sem=g_recv.at[slot, part],
                device_id={"mp": dest},
                device_id_type=MESH,
            ).start()

    def arrive(slot, part):
        wait_bytes(chunks.at[slot, part], g_recv.at[slot, part])

    def whole(slot):
        return chunks[slot].reshape(TOK, WIDE)

    def consume(slot):
        thru[...] += dot_nt(whole(slot), a2_cut[slot])

    sibling = at(h, x, s)
    fore, back = at(h, ahead, c), at(h, behind, c)
    for part in range(PARTS):
        send(mm, part, at(o, x, c))
    for part in range(PARTS):
        send(mm, part, fore, back)
    for part in range(PARTS):
        send(mm, part, sibling)
    thru[...] = dot_nt(packed, a2_cut[mm])

    def second_factor():
        wait_bytes(low_all.at[pl.ds(0, MP - 1)], lg_recv)
        low = low_all[...].reshape(MP * 16, RW)[:TOK, :]
        b_part[...] = dot_tn(low, packed)
        for k in range(DP):
            b_out[k] = b_part[2 * k : 2 * k + 2, :]
        b_in[me] = b_out[me]
        over_dp(b_out, b_in, b_send, b_recv)

    def neighbours(hh):
        for part in range(PARTS):
            arrive(at(hh, behind, c), part)
            on = (fore, sibling) if hh is h else (fore, at(h, ahead, s), sibling)
            send(at(hh, behind, c), part, *on)
        for part in range(PARTS):
            arrive(at(hh, ahead, c), part)
            send(at(hh, ahead, c), part, sibling)

    def last(hh, part):
        arrive(at(hh, across, c), part)
        if hh is h:
            send(at(hh, across, c), part, sibling)

    def add(hh):
        for xx in (behind, ahead, across):
            consume(at(hh, xx, c))
        for xx in (x, ahead, behind, across):
            for part in range(PARTS):
                arrive(at(hh, xx, s), part)
            consume(at(hh, xx, s))

    neighbours(h)
    for part in range(PARTS):
        arrive(at(o, x, c), part)
        send(at(o, x, c), part, fore, back, sibling)
        last(h, part)
    second_factor()
    neighbours(o)
    consume(at(o, x, c))
    add(h)
    for part in range(PARTS):
        last(o, part)
    add(o)

    through = thru[...].astype(BF16)
    a_out[...] = dot_nn(hidden_t[...], through).astype(BF16).reshape(DP, 16, RW)
    a_in[me] = a_out[me]
    over_dp(a_out, a_in, r_send, r_recv)

    wait_bytes(b_in.at[pl.ds(0, DP - 1)], b_recv)
    b_all[mm] = jnp.sum(b_in[...], axis=0)
    over_mp(b_all, b_all, bg_send, bg_recv, False)

    acc[...] = dot_nn(through[:, :RANK], a1[...])

    @pl.loop(0, MP)
    def _(k):
        acc[...] += dot_nt(whole(k), w_cut[k])

    grad_hidden = acc[...]
    gg[...] = (grad_hidden * c_gate[...]).astype(BF16)
    gu[...] = (grad_hidden * c_up[...]).astype(BF16)

    wait_bytes(b_all.at[pl.ds(0, MP - 1)], bg_recv)
    for k in range(MP):
        gb_ref[:, k * FEAT : (k + 1) * FEAT] = b_all[k][:, :FEAT]

    wait_bytes(slots_out.at[pl.ds(0, DP - 1)], p_send)
    wait_bytes(low_out.at[pl.ds(0, MP - 1)], l_send)
    wait_bytes(low_all.at[pl.ds(0, MP - 1)], lg_send)
    wait_bytes(chunks.at[pl.ds(0, MP - 1)], g_send)
    wait_bytes(b_out.at[pl.ds(0, DP - 1)], b_send)
    wait_bytes(b_all.at[pl.ds(0, MP - 1)], bg_send)
    wait_bytes(a_in.at[pl.ds(0, DP - 1)], r_recv)
    total = jnp.sum(a_in[...].astype(F32), axis=0)
    ga_ref[...] = total[:PIECE, :RANK].reshape(PIECE, 1, RANK)
    wait_bytes(a_out.at[pl.ds(0, DP - 1)], r_send)


def deliver(*refs):
    sources, targets, sem = refs[:4], refs[4:8], refs[8]
    copies = [
        pltpu.make_async_copy(source, target, sem.at[k])
        for k, (source, target) in enumerate(zip(sources, targets))
    ]
    for copy in copies:
        copy.start()
    for copy in copies:
        copy.wait()


def body(og, gate, up, w, a1, a2, plan):
    hbm = pl.BlockSpec(memory_space=pltpu.HBM)
    vmem = pl.BlockSpec(memory_space=pltpu.VMEM)
    V = pltpu.VMEM
    results = (
        jax.ShapeDtypeStruct((TOK, HID), BF16),
        jax.ShapeDtypeStruct((TOK, HID), BF16),
        jax.ShapeDtypeStruct((PIECE, 1, RANK), F32),
        jax.ShapeDtypeStruct((2, MODEL), F32),
    )
    found = pl.pallas_call(
        kernel,
        out_shape=results,
        in_specs=[hbm] * 7,
        out_specs=(vmem,) * 4,
        scratch_shapes=[
            V((TOK, FEAT), BF16),
            V((TOK, WIDE), BF16),
            V((TOK, HID), BF16),
            V((TOK, HID), BF16),
            V((HID, MODEL), BF16),
            V((RANK, HID), BF16),
            V((RANK, MODEL), BF16),
            V((1, 24), jnp.int32),
            V((DP, 8, WIDE), BF16),
            V((DP, 8, WIDE), BF16),
            V((MP, 16, RW), BF16),
            V((MP, 16, RW), BF16),
            V((MP, 16, RW), BF16),
            V((MP, PARTS, TOK // PARTS, WIDE), BF16),
            V((MP, RW, WIDE), BF16),
            V((MP, HID, WIDE), BF16),
            V((TOK, RW), F32),
            V((TOK, HID), F32),
            V((TOK, HID), F32),
            V((TOK, HID), F32),
            V((DP * 16, TOK), BF16),
            V((DP * 8, DP * 8), BF16),
            V((RW, WIDE), F32),
            V((DP, 2, WIDE), F32),
            V((DP, 2, WIDE), F32),
            V((MP, 2, WIDE), F32),
            V((DP, 16, RW), BF16),
            V((DP, 16, RW), BF16),
            pltpu.SemaphoreType.DMA((7,)),
            pltpu.SemaphoreType.DMA((MP, PARTS)),
            pltpu.SemaphoreType.DMA((13,)),
        ],
        compiler_params=pltpu.CompilerParams(
            collective_id=0, has_side_effects=True, vmem_limit_bytes=48 * 1024 * 1024
        ),
        name="repack_backward",
    )(*[
        pltpu.with_memory_space_constraint(v, pltpu.HBM)
        for v in (og, gate, up, w, a1.T, a2, plan.reshape(1, 24))
    ])
    gg, gu, ga, gb = pl.pallas_call(
        deliver,
        out_shape=results,
        in_specs=[vmem] * 4,
        out_specs=(hbm,) * 4,
        scratch_shapes=[pltpu.SemaphoreType.DMA((4,))],
        compiler_params=pltpu.CompilerParams(vmem_limit_bytes=1024 * 1024),
        name="deliver",
    )(*found)
    return gg, gu, ga.reshape(1, PIECE, RANK), gb


def solution(mesh):
    return jax.shard_map(
        body,
        mesh=mesh,
        in_specs=(
            P("dp", "mp"),
            P("dp", "mp"),
            P("dp", "mp"),
            P("mp", None),
            P("mp", None),
            P(),
            P("dp"),
        ),
        out_specs=(P("dp", "mp"), P("dp", "mp"), P("mp", "dp", None), P("dp", None)),
        check_vma=False,
    )
```
